32 devices in a mesh: cp: 8 (over y, x, core), tp: 4 (over z).
Axes of the slice: x: 2, y: 2, z: 4, core: 2. Of those that a mesh axis runs over, the one named last changes fastest.
Arguments:
- queries: bfloat16 [6144, 5120], P('cp', 'tp'), may hold values from -36 to 36
- keys: bfloat16 [6144, 1024], P('cp', 'tp'), may hold values from -5 to 5
- values: bfloat16 [6144, 1024], P('cp', 'tp'), may hold values from -6 to 6
- doc_lengths: int32 [8], replicated, may hold values from 1 to 1536, 6144 in all
Outputs:
- attended: bfloat16 [6144, 5120], P(('cp', 'tp'))
The draws below stay inside these ranges and needn't reach their ends.
Inputs may be any that keep to these rules, and one draw needn't show every extreme that they name: `doc_lengths`: they sum to 6144, and one of them is exactly 1536.
All inputs are finite; a program needn't handle non-finite values.
Results may differ from the reference program's by a relative error of at most 0.0038.
Values may be sent and summed in bfloat16 or wider, within the bound.
A program may use at most 256 MiB of HBM per device.

```python
import math
import jax
import jax.numpy as jnp
import numpy as np
from jax import lax

Q_HEADS = 40
KV_HEADS = 8
HEAD = 128
TOK_DEV = 768
TOKENS = 6144
MAXDOC = 1536
NDOCS = 8
N_CP = 8


def draw_keys(key, part):
    drawn_draw = jnp.clip(jax.random.normal(jax.random.fold_in(key, 11), (TOKENS, KV_HEADS, HEAD), jnp.float32), -5.0, 5.0)
    result = drawn_draw
    return result.reshape(TOKENS, KV_HEADS * HEAD).astype(jnp.bfloat16)


def draw_queries(key, part):
    group_size = Q_HEADS // KV_HEADS
    drawn_draw = jnp.clip(jax.random.normal(jax.random.fold_in(key, 12), (TOKENS, KV_HEADS, group_size, HEAD), jnp.float32), -5.0, 5.0)
    result = drawn_draw
    return result.reshape(TOKENS, Q_HEADS * HEAD).astype(jnp.bfloat16)


def shard_levels(key, dims, split, low, largest):
    loudness, own = 1.0, jax.random.fold_in(key, 6)
    for dim, blocks in split:
        steps = jnp.exp(jax.random.uniform(jax.random.fold_in(own, dim), (blocks,), jnp.float32, low / len(split), largest / len(split)))
        loudness = loudness * jnp.repeat(steps, dims[dim] // blocks).reshape([-1 if axis == dim else 1 for axis in range(len(dims))])
    return loudness


def length_profile(number_of, total, most, slope):
    loads = [(1 << 20) // math.isqrt(standing ** slope) + 1 for standing in range(2, number_of + 1)]
    spare, counts = total - most - (number_of - 1), [1] * (number_of - 1)
    while spare > 0:
        candidates = [i for i in range(number_of - 1) if counts[i] < most]
        mass, left = sum([loads[i] for i in candidates]), spare
        for i in candidates:
            extra = min(most - counts[i], max(1, left * loads[i] // mass), spare)
            counts[i] = counts[i] + extra
            spare = spare - extra
    return np.array([most] + counts)


def ragged_sizes(own_key, amount, total, reach, skew):
    if amount == 2:
        one = jax.random.randint(own_key, (), max(1, total - reach), min(reach, total - 1) + 1)
        return jnp.stack([one, total - one])
    tallies = jnp.asarray(length_profile(amount, total, reach, skew), jnp.int32)
    twos = (amount - 1) // 2
    donor, receiver = tallies[1:1 + 2 * twos:2], tallies[2:2 + 2 * twos:2]
    margin = jnp.minimum(donor - 1, reach - receiver)
    passed = jax.random.randint(jax.random.fold_in(own_key, 1), (twos,), 0, 1 << 20) % (margin + 1)
    tallies = tallies.at[1:1 + 2 * twos:2].set(donor - passed).at[2:2 + 2 * twos:2].set(receiver + passed)
    return tallies[jax.random.permutation(jax.random.fold_in(own_key, 2), amount)]


def bell_draw(own_key, extent, width, most, split=(), held_as=jnp.bfloat16):
    values = jax.random.normal(own_key, extent, jnp.float32) * width
    if len(split) > 0:
        values = shard_levels(own_key, extent, split, -0.22, 0.18) * values
    return jnp.clip(values, min=-most, max=most).astype(held_as)


def setup_inputs(seed: int = 0) -> dict:
    splits = jax.random.split(jax.random.key(seed), 5)
    return {
        "queries": draw_queries(jax.random.fold_in(splits[4], 71), 0),
        "keys": draw_keys(jax.random.fold_in(splits[4], 71), 0),
        "values": bell_draw(splits[2], (TOKENS, KV_HEADS * HEAD), 1.0, 6.0, ((0, 8), (1, 4))),
        "doc_lengths": ragged_sizes(splits[3], NDOCS, TOKENS, MAXDOC, 2).astype(jnp.int32),
    }


negative = -1.0e30


def to_sequence(blocked):
    key_width = blocked.shape[1]
    parts = blocked.reshape(N_CP, 2, TOK_DEV // 2, key_width)
    return jnp.concatenate([parts[:, 0], parts[::-1, 1]], axis=0).reshape(TOKENS, key_width)


def reference(queries, keys, values, doc_lengths):
    half_rows = TOK_DEV // 2
    group_size = Q_HEADS // KV_HEADS
    seq_queries = to_sequence(queries).reshape(TOKENS, KV_HEADS, group_size, HEAD)
    seq_keys = to_sequence(keys).reshape(TOKENS, KV_HEADS, HEAD)
    seq_values = to_sequence(values).reshape(TOKENS, KV_HEADS, HEAD)
    doc_ends = jnp.cumsum(doc_lengths).astype(jnp.int32)
    positions = jnp.arange(TOKENS, dtype=jnp.int32)
    doc_ids = jnp.sum((positions[:, None] >= doc_ends[None, :]).astype(jnp.int32), axis=1).astype(jnp.int32)
    padded_keys = jnp.concatenate([jnp.zeros((MAXDOC, KV_HEADS, HEAD), seq_keys.dtype), seq_keys], axis=0)
    padded_values = jnp.concatenate([jnp.zeros((MAXDOC, KV_HEADS, HEAD), seq_values.dtype), seq_values], axis=0)
    padded_docs = jnp.concatenate([jnp.full((MAXDOC,), -1, jnp.int32), doc_ids], axis=0)
    key_width = MAXDOC + half_rows
    scale = float(HEAD) ** -0.5

    def one_block(block_index):
        row_start = (block_index * half_rows).astype(jnp.int32)
        query_block = lax.dynamic_slice_in_dim(seq_queries, row_start, half_rows, 0)
        key_block = lax.dynamic_slice_in_dim(padded_keys, row_start, key_width, 0)
        value_block = lax.dynamic_slice_in_dim(padded_values, row_start, key_width, 0)
        q_doc = lax.dynamic_slice_in_dim(doc_ids, row_start, half_rows, 0)
        k_doc = lax.dynamic_slice_in_dim(padded_docs, row_start, key_width, 0)
        q_pos = row_start + jnp.arange(half_rows, dtype=jnp.int32)
        k_pos = row_start - MAXDOC + jnp.arange(key_width, dtype=jnp.int32)
        allowed = (k_doc[None, :] == q_doc[:, None]) & (k_pos[None, :] <= q_pos[:, None])
        scores = jnp.einsum("qhjd,khd->qhjk", query_block.astype(jnp.float32), key_block.astype(jnp.float32)) * scale
        allowed_wide = allowed[:, None, None, :]
        masked = jnp.where(allowed_wide, scores, negative)
        row_max = jnp.max(masked, axis=-1, keepdims=True)
        weights = jnp.where(allowed_wide, jnp.exp(masked - row_max), 0.0)
        weight_sum = jnp.sum(weights, axis=-1)
        rounded = lax.optimization_barrier(weights.astype(jnp.bfloat16)).astype(jnp.float32)
        output = jnp.einsum("qhjk,khd->qhjd", rounded, value_block.astype(jnp.float32)) / weight_sum[..., None]
        return output.astype(jnp.bfloat16)

    blocks = lax.map(one_block, jnp.arange(2 * N_CP, dtype=jnp.int32))
    flattened = blocks.reshape(2 * N_CP, half_rows, Q_HEADS * HEAD)
    first_half = flattened[:N_CP]
    second_half = flattened[N_CP:][::-1]
    return jnp.stack([first_half, second_half], axis=1).reshape(TOKENS, Q_HEADS * HEAD)
```

```python
import functools
import math

import jax
import jax.numpy as jnp
from jax import lax
from jax.experimental import pallas as pl
from jax.experimental.pallas import tpu as pltpu
from jax.sharding import PartitionSpec as P

HEAD = 128
BACK = 4
LANES = 128
negative = -1e30
MESH = pl.DeviceIdType.MESH


def kernel(
    n_cp, n_tp, group, kv_local,
    doc_ref, q_ref, k_ref, v_ref, out_ref,
    kbuf, vbuf, bias_ref, s_ref, mx_ref, p_ref, obuf,
    own_send, relay_send, kv_recv, o_send, o_recv,
):
    tok = q_ref.shape[0]
    half = tok // 2
    rows = tok // n_tp
    parts = half // rows
    window = bias_ref.shape[2]
    step = half * (BACK + 1) - window
    step = step // max(parts - 1, 1)
    cols = group * HEAD
    me = lax.axis_index("cp")
    tp = lax.axis_index("tp")
    core = me % 2
    chip = me // 2
    chips = n_cp // 2
    partner = me + 1 - 2 * core
    bufs = (kbuf, vbuf)
    srcs = (k_ref, v_ref)
    idx = (core, 1 - core)

    def part(kv, h, g, slot):
        return bufs[kv][g].at[h, pl.ds(pl.multiple_of(slot * half, half), half)]

    def src(kv, h, g):
        return srcs[kv].at[pl.ds(h * half, half), pl.ds(g * HEAD, HEAD)]

    def send(source, kv, h, g, slot, ssem, dev):
        return pltpu.make_async_remote_copy(
            src_ref=source,
            dst_ref=part(kv, h, g, slot),
            send_sem=ssem,
            recv_sem=kv_recv.at[kv, h, g, slot],
            device_id={"cp": dev},
            device_id_type=MESH,
        )

    routes = []
    for o in (2, 1):
        base = (2 - o) * 2
        routes.append((0, o, chip + o <= chips - 1, chip + o, 0, base + idx[0]))
        if o == 2:
            routes.append((0, o, chip == chips - 1, chips - 2, 1, base + idx[0]))
        routes.append((1, o, chip >= o, chip - o, 1, base + idx[1]))

    def own_copies(g, fn):
        for kv in range(2):
            for h, o, when, tchip, thalf, slot in routes:
                @pl.when(when)
                def _(kv=kv, h=h, o=o, tchip=tchip, thalf=thalf, slot=slot):
                    fn(send(src(kv, h, g), kv, thalf, g, slot, own_send.at[kv, h, g, o], 2 * tchip + core))
            for h in range(2):
                fn(send(src(kv, h, g), kv, h, g, 4 + idx[h], own_send.at[kv, h, g, 0], partner))

    arrivals = []
    for o in (2, 1):
        arrivals.append((0, o, chip >= o, core))
        arrivals.append((1, o, chip < chips - o, 1 - core))
        if o == 2:
            arrivals.append((1, o, chip == chips - 2, core))

    def relays(g, fn):
        for h, o, when, r in arrivals:
            @pl.when(when)
            def _(h=h, o=o, r=r):
                for kv in range(2):
                    slot = (2 - o) * 2 + r
                    fn(send(part(kv, h, g, slot), kv, h, g, slot, relay_send.at[kv, h, g, o], partner))

    def take(copy):
        copy.wait_recv()
        copy.start()

    def relay_arrivals(g):
        for h, o, when, r in arrivals:
            @pl.when(when)
            def _(h=h, o=o, r=r):
                for kv in range(2):
                    slot = (2 - o) * 2 + 1 - r
                    send(part(kv, h, g, slot), kv, h, g, slot, relay_send.at[kv, h, g, o], partner).wait_recv()
        for h in range(2):
            for kv in range(2):
                slot = 4 + 1 - idx[h]
                send(part(kv, h, g, slot), kv, h, g, slot, own_send.at[kv, h, g, 0], partner).wait_recv()

        @pl.when(chip == chips - 1)
        def _():
            for buf in bufs:
                buf[g][1, 0:4 * half] = buf[g][0, 2 * half:6 * half]

    for g in range(kv_local):
        own_copies(g, lambda copy: copy.start())

    for g in range(kv_local):
        for h in range(2):
            for kv in range(2):
                part(kv, h, g, 4 + idx[h])[...] = srcs[kv][h * half:(h + 1) * half, g * HEAD:(g + 1) * HEAD]
        for lowest in range(2):
            @pl.when(chip <= lowest)
            def _(g=g, lowest=lowest):
                first = 2 if lowest == 0 else 0
                for buf in bufs:
                    buf[g][0, first * half:(first + 2) * half] = jnp.zeros((2 * half, HEAD), jnp.bfloat16)

    def place(u):
        h = u // parts
        i = u % parts
        pair = chip + h * (2 * chips - 1 - 2 * chip)
        index = core + h * (1 - 2 * core)
        return h, i, pair, index

    def make_bias(u, _):
        h, i, pair, index = place(u)
        block = 2 * pair + index
        q_pos = block * half + i * rows + lax.broadcasted_iota(jnp.int32, (rows, LANES), 0)

        def doc_step(j, carry):
            end, low = carry
            end = end + doc_ref[j]
            return end, jnp.where(end <= q_pos, end, low)

        _, low = lax.fori_loop(0, doc_ref.shape[0], doc_step, (jnp.int32(0), jnp.zeros((rows, LANES), jnp.int32)))
        first = (block - BACK) * half + i * step
        for tile in range(window // LANES):
            k_pos = first + tile * LANES + lax.broadcasted_iota(jnp.int32, (rows, LANES), 1)
            ok = (k_pos >= low) & (k_pos <= q_pos)
            bias_ref[u, :, tile * LANES:(tile + 1) * LANES] = jnp.where(ok, 0.0, negative)
        return 0

    lax.fori_loop(0, n_tp, make_bias, 0)

    chunk = 2 * LANES
    factor = float(HEAD) ** -0.5 * math.log2(math.e)

    def out_copy(g, u):
        return pltpu.make_async_remote_copy(
            src_ref=obuf.at[g, u],
            dst_ref=out_ref.at[:, pl.ds(pl.multiple_of(tp * (kv_local * cols) + g * cols, LANES), cols)],
            send_sem=o_send.at[g, u],
            recv_sem=o_recv.at[g, tp],
            device_id={"tp": u},
            device_id_type=MESH,
        )

    def out_arrival(g, source):
        return pltpu.make_async_remote_copy(
            src_ref=obuf.at[g, source],
            dst_ref=out_ref.at[:, pl.ds(pl.multiple_of(source * (kv_local * cols) + g * cols, LANES), cols)],
            send_sem=o_send.at[g, source],
            recv_sem=o_recv.at[g, source],
            device_id={"tp": source},
            device_id_type=MESH,
        )

    def attend(g, u):
        h, i, pair, index = place(u)
        row0 = pl.multiple_of(u * rows, 16)
        q = jnp.concatenate(
            [q_ref[pl.ds(row0, rows), (g * group + j) * HEAD:(g * group + j + 1) * HEAD] for j in range(group)], axis=0
        )
        start = index * half + i * step
        mx_ref[...] = jnp.full(mx_ref.shape, negative, jnp.float32)

        def score_chunk(kc, _):
            k = kbuf[g][h, pl.ds(pl.multiple_of(start + kc * chunk, LANES), chunk), :]
            s = lax.dot_general(q, k, (((1,), (1,)), ((), ())), preferred_element_type=jnp.float32)
            at = pl.ds(pl.multiple_of(kc * chunk, chunk), chunk)
            bias = bias_ref[u, :, at]
            for j in range(group):
                here = slice(j * rows, (j + 1) * rows)
                sj = s[here] + bias
                s_ref[here, at] = sj
                mx_ref[here] = jnp.maximum(mx_ref[here], jnp.maximum(sj[:, :LANES], sj[:, LANES:]))
            return 0

        lax.fori_loop(0, window // chunk, score_chunk, 0)
        tall = 64

        def weigh(rc, _):
            at = pl.ds(pl.multiple_of(rc * tall, tall), tall)
            top = jnp.max(mx_ref[at, :], axis=1, keepdims=True)
            p_ref[at, :] = jnp.exp2((s_ref[at, :] - top) * factor).astype(jnp.bfloat16)
            return 0

        lax.fori_loop(0, group * rows // tall, weigh, 0)
        v = vbuf[g][h, pl.ds(pl.multiple_of(start, LANES), window), :]
        wide = jnp.concatenate([v, jnp.ones_like(v)], axis=1)
        acc = jnp.dot(p_ref[...], wide, preferred_element_type=jnp.float32)
        done = (acc[:, :HEAD] / acc[:, HEAD:]).astype(jnp.bfloat16)
        for j in range(group):
            obuf[g, u, :, j * HEAD:(j + 1) * HEAD] = done[j * rows:(j + 1) * rows]

    relays(0, take)
    relay_arrivals(0)
    for g in range(kv_local):
        def one(k, _, g=g):
            u = (tp + 1 + k) % n_tp
            if g + 1 < kv_local:
                @pl.when(k == n_tp - 1)
                def _():
                    relays(g + 1, take)
            attend(g, u)

            @pl.when(k < n_tp - 1)
            def _():
                out_copy(g, u).start()
            return 0

        lax.fori_loop(0, n_tp, one, 0)
        out_ref[:, pl.ds(pl.multiple_of(tp * (kv_local * cols) + g * cols, LANES), cols)] = obuf[g, tp]
        if g + 1 < kv_local:
            relay_arrivals(g + 1)

    for g in range(kv_local):
        own_copies(g, lambda copy: copy.wait_send())
        relays(g, lambda copy: copy.wait_send())

        def finish(k, _, g=g):
            u = (tp + 1 + k) % n_tp
            out_copy(g, u).wait_send()
            out_arrival(g, u).wait_recv()
            return 0

        lax.fori_loop(0, n_tp - 1, finish, 0)


def on_device(queries, keys, values, doc_lengths):
    tok, q_cols = queries.shape
    kv_local = keys.shape[1] // HEAD
    group = q_cols // keys.shape[1]
    n_cp = lax.axis_size("cp")
    n_tp = lax.axis_size("tp")
    half = tok // 2
    rows = tok // n_tp
    window = -(-(BACK * half + rows) // (2 * LANES)) * 2 * LANES
    vmem = pl.BlockSpec(memory_space=pltpu.VMEM)
    dma = pltpu.SemaphoreType.DMA
    halo = (pltpu.VMEM((2, 6 * half, HEAD), jnp.bfloat16),) * kv_local
    return pl.pallas_call(
        functools.partial(kernel, n_cp, n_tp, group, kv_local),
        out_shape=jax.ShapeDtypeStruct((rows, q_cols * n_tp), jnp.bfloat16),
        in_specs=[pl.BlockSpec(memory_space=pltpu.SMEM), vmem, vmem, vmem],
        out_specs=vmem,
        scratch_shapes=[
            halo,
            halo,
            pltpu.VMEM((n_tp, rows, window), jnp.float32),
            pltpu.VMEM((group * rows, window), jnp.float32),
            pltpu.VMEM((group * rows, LANES), jnp.float32),
            pltpu.VMEM((group * rows, window), jnp.bfloat16),
            pltpu.VMEM((kv_local, n_tp, rows, group * HEAD), jnp.bfloat16),
            dma((2, 2, kv_local, 3)),
            dma((2, 2, kv_local, 3)),
            dma((2, 2, kv_local, 6)),
            dma((kv_local, n_tp)),
            dma((kv_local, n_tp)),
        ],
        compiler_params=pltpu.CompilerParams(has_side_effects=True, vmem_limit_bytes=60 * 1024 * 1024),
    )(doc_lengths, queries, keys, values)


def solution(mesh):
    in_specs = (P("cp", "tp"), P("cp", "tp"), P("cp", "tp"), P())
    return jax.shard_map(
        on_device, mesh=mesh, in_specs=in_specs, out_specs=P(("cp", "tp"), None), check_vma=False
    )
```

```python
import functools
import math

import jax
import jax.numpy as jnp
from jax import lax
from jax.experimental import pallas as pl
from jax.experimental.pallas import tpu as pltpu
from jax.sharding import PartitionSpec as P

HEAD = 128
BACK = 4
LANES = 128
negative = -1e30
MESH = pl.DeviceIdType.MESH


def kernel(
    n_cp, n_tp, group, kv_local,
    doc_ref, q_ref, k_ref, v_ref, out_ref,
    kbuf, vbuf, bias_ref, s_ref, mx_ref, p_ref, obuf,
    own_send, relay_send, kv_recv, o_send, o_recv,
):
    tok = q_ref.shape[0]
    half = tok // 2
    rows = tok // n_tp
    parts = half // rows
    window = bias_ref.shape[2]
    step = half * (BACK + 1) - window
    step = step // max(parts - 1, 1)
    cols = group * HEAD
    me = lax.axis_index("cp")
    tp = lax.axis_index("tp")
    core = me % 2
    chip = me // 2
    chips = n_cp // 2
    partner = me + 1 - 2 * core
    bufs = (kbuf, vbuf)
    srcs = (k_ref, v_ref)
    idx = (core, 1 - core)

    def part(kv, h, g, slot):
        return bufs[kv][g].at[h, pl.ds(pl.multiple_of(slot * half, half), half)]

    def src(kv, h, g):
        return srcs[kv].at[pl.ds(h * half, half), pl.ds(g * HEAD, HEAD)]

    def send(source, kv, h, g, slot, ssem, dev):
        return pltpu.make_async_remote_copy(
            src_ref=source,
            dst_ref=part(kv, h, g, slot),
            send_sem=ssem,
            recv_sem=kv_recv.at[kv, h, g, slot],
            device_id={"cp": dev},
            device_id_type=MESH,
        )

    routes = []
    for o in (2, 1):
        base = (2 - o) * 2
        routes.append((0, o, chip + o <= chips - 1, chip + o, 0, base + idx[0]))
        if o == 2:
            routes.append((0, o, chip == chips - 1, chips - 2, 1, base + idx[0]))
        routes.append((1, o, chip >= o, chip - o, 1, base + idx[1]))

    def own_copies(g, fn):
        for kv in range(2):
            for h, o, when, tchip, thalf, slot in routes:
                @pl.when(when)
                def _(kv=kv, h=h, o=o, tchip=tchip, thalf=thalf, slot=slot):
                    fn(send(src(kv, h, g), kv, thalf, g, slot, own_send.at[kv, h, g, o], 2 * tchip + core))
            for h in range(2):
                fn(send(src(kv, h, g), kv, h, g, 4 + idx[h], own_send.at[kv, h, g, 0], partner))

    arrivals = []
    for o in (2, 1):
        arrivals.append((0, o, chip >= o, core))
        arrivals.append((1, o, chip < chips - o, 1 - core))
        if o == 2:
            arrivals.append((1, o, chip == chips - 2, core))

    def relays(g, fn):
        for h, o, when, r in arrivals:
            @pl.when(when)
            def _(h=h, o=o, r=r):
                for kv in range(2):
                    slot = (2 - o) * 2 + r
                    fn(send(part(kv, h, g, slot), kv, h, g, slot, relay_send.at[kv, h, g, o], partner))

    def take(copy):
        copy.wait_recv()
        copy.start()

    def relay_arrivals(g):
        for h, o, when, r in arrivals:
            @pl.when(when)
            def _(h=h, o=o, r=r):
                for kv in range(2):
                    slot = (2 - o) * 2 + 1 - r
                    send(part(kv, h, g, slot), kv, h, g, slot, relay_send.at[kv, h, g, o], partner).wait_recv()
        for h in range(2):
            for kv in range(2):
                slot = 4 + 1 - idx[h]
                send(part(kv, h, g, slot), kv, h, g, slot, own_send.at[kv, h, g, 0], partner).wait_recv()

        @pl.when(chip == chips - 1)
        def _():
            for buf in bufs:
                buf[g][1, 0:4 * half] = buf[g][0, 2 * half:6 * half]

    barrier = pltpu.get_barrier_semaphore()
    greeted = n_tp
    pl.semaphore_signal(barrier, inc=1, device_id={"cp": partner}, device_id_type=MESH)
    for other in range(1, n_tp):
        pl.semaphore_signal(barrier, inc=1, device_id={"tp": (tp + other) % n_tp}, device_id_type=MESH)
    for away in (-2, -1, 1, 2):
        there = chip + away
        inside = (there >= 0) & (there < chips)
        greeted = greeted + inside.astype(jnp.int32)

        @pl.when(inside)
        def _(there=there):
            pl.semaphore_signal(barrier, inc=1, device_id={"cp": 2 * there + core}, device_id_type=MESH)
    pl.semaphore_wait(barrier, greeted)

    own_copies(0, lambda copy: copy.start())

    for g in range(kv_local):
        for h in range(2):
            for kv in range(2):
                part(kv, h, g, 4 + idx[h])[...] = srcs[kv][h * half:(h + 1) * half, g * HEAD:(g + 1) * HEAD]
        for lowest in range(2):
            @pl.when(chip <= lowest)
            def _(g=g, lowest=lowest):
                first = 2 if lowest == 0 else 0
                for buf in bufs:
                    buf[g][0, first * half:(first + 2) * half] = jnp.zeros((2 * half, HEAD), jnp.bfloat16)

    def place(u):
        h = u // parts
        i = u % parts
        pair = chip + h * (2 * chips - 1 - 2 * chip)
        index = core + h * (1 - 2 * core)
        return h, i, pair, index

    def make_bias(u, _):
        h, i, pair, index = place(u)
        block = 2 * pair + index
        q_pos = block * half + i * rows + lax.broadcasted_iota(jnp.int32, (rows, LANES), 0)

        def doc_step(j, carry):
            end, low = carry
            end = end + doc_ref[j]
            return end, jnp.where(end <= q_pos, end, low)

        _, low = lax.fori_loop(0, doc_ref.shape[0], doc_step, (jnp.int32(0), jnp.zeros((rows, LANES), jnp.int32)))
        first = (block - BACK) * half + i * step
        for tile in range(window // LANES):
            k_pos = first + tile * LANES + lax.broadcasted_iota(jnp.int32, (rows, LANES), 1)
            ok = (k_pos >= low) & (k_pos <= q_pos)
            bias_ref[u, :, tile * LANES:(tile + 1) * LANES] = jnp.where(ok, 0.0, negative)
        return 0

    lax.fori_loop(0, n_tp, make_bias, 0)

    chunk = 2 * LANES
    factor = float(HEAD) ** -0.5 * math.log2(math.e)

    def out_copy(g, u):
        return pltpu.make_async_remote_copy(
            src_ref=obuf.at[g, u],
            dst_ref=out_ref.at[:, pl.ds(pl.multiple_of(tp * (kv_local * cols) + g * cols, LANES), cols)],
            send_sem=o_send.at[g, u],
            recv_sem=o_recv.at[g, tp],
            device_id={"tp": u},
            device_id_type=MESH,
        )

    def out_arrival(g, source):
        return pltpu.make_async_remote_copy(
            src_ref=obuf.at[g, source],
            dst_ref=out_ref.at[:, pl.ds(pl.multiple_of(source * (kv_local * cols) + g * cols, LANES), cols)],
            send_sem=o_send.at[g, source],
            recv_sem=o_recv.at[g, source],
            device_id={"tp": source},
            device_id_type=MESH,
        )

    def attend(g, u):
        h, i, pair, index = place(u)
        row0 = pl.multiple_of(u * rows, 16)
        q = jnp.concatenate(
            [q_ref[pl.ds(row0, rows), (g * group + j) * HEAD:(g * group + j + 1) * HEAD] for j in range(group)], axis=0
        )
        start = index * half + i * step
        mx_ref[...] = jnp.full(mx_ref.shape, negative, jnp.float32)

        def score_chunk(kc, _):
            k = kbuf[g][h, pl.ds(pl.multiple_of(start + kc * chunk, LANES), chunk), :]
            s = lax.dot_general(q, k, (((1,), (1,)), ((), ())), preferred_element_type=jnp.float32)
            at = pl.ds(pl.multiple_of(kc * chunk, chunk), chunk)
            bias = bias_ref[u, :, at]
            for j in range(group):
                here = slice(j * rows, (j + 1) * rows)
                sj = s[here] + bias
                s_ref[here, at] = sj
                mx_ref[here] = jnp.maximum(mx_ref[here], jnp.maximum(sj[:, :LANES], sj[:, LANES:]))
            return 0

        lax.fori_loop(0, window // chunk, score_chunk, 0)
        tall = 64

        def weigh(rc, _):
            at = pl.ds(pl.multiple_of(rc * tall, tall), tall)
            top = jnp.max(mx_ref[at, :], axis=1, keepdims=True)
            p_ref[at, :] = jnp.exp2((s_ref[at, :] - top) * factor).astype(jnp.bfloat16)
            return 0

        lax.fori_loop(0, group * rows // tall, weigh, 0)
        v = vbuf[g][h, pl.ds(pl.multiple_of(start, LANES), window), :]
        wide = jnp.concatenate([v, jnp.ones_like(v)], axis=1)
        acc = jnp.dot(p_ref[...], wide, preferred_element_type=jnp.float32)
        done = (acc[:, :HEAD] / acc[:, HEAD:]).astype(jnp.bfloat16)
        for j in range(group):
            obuf[g, u, :, j * HEAD:(j + 1) * HEAD] = done[j * rows:(j + 1) * rows]

    def order(k):
        if n_tp != 4:
            return (tp + 1 + k) % n_tp
        far = (tp // 2 + 1 - k // 2) % 2
        return 2 * far + (tp % 2 + k + k // 2) % 2

    relays(0, take)
    for g in range(1, kv_local):
        own_copies(g, lambda copy: copy.start())
    relay_arrivals(0)
    for g in range(kv_local):
        def one(k, _, g=g):
            u = order(k)
            if g + 1 < kv_local:
                @pl.when(k == n_tp - 1)
                def _():
                    relays(g + 1, take)
            attend(g, u)

            @pl.when(k < n_tp - 1)
            def _():
                out_copy(g, u).start()
            return 0

        lax.fori_loop(0, n_tp, one, 0)
        out_ref[:, pl.ds(pl.multiple_of(tp * (kv_local * cols) + g * cols, LANES), cols)] = obuf[g, tp]
        if g + 1 < kv_local:
            relay_arrivals(g + 1)

    for g in range(kv_local):
        own_copies(g, lambda copy: copy.wait_send())
        relays(g, lambda copy: copy.wait_send())

        def finish(k, _, g=g):
            u = (tp + 1 + k) % n_tp
            out_copy(g, u).wait_send()
            out_arrival(g, u).wait_recv()
            return 0

        lax.fori_loop(0, n_tp - 1, finish, 0)


def on_device(queries, keys, values, doc_lengths):
    tok, q_cols = queries.shape
    kv_local = keys.shape[1] // HEAD
    group = q_cols // keys.shape[1]
    n_cp = lax.axis_size("cp")
    n_tp = lax.axis_size("tp")
    half = tok // 2
    rows = tok // n_tp
    window = -(-(BACK * half + rows) // (2 * LANES)) * 2 * LANES
    vmem = pl.BlockSpec(memory_space=pltpu.VMEM)
    dma = pltpu.SemaphoreType.DMA
    halo = (pltpu.VMEM((2, 6 * half, HEAD), jnp.bfloat16),) * kv_local
    return pl.pallas_call(
        functools.partial(kernel, n_cp, n_tp, group, kv_local),
        out_shape=jax.ShapeDtypeStruct((rows, q_cols * n_tp), jnp.bfloat16),
        in_specs=[pl.BlockSpec(memory_space=pltpu.SMEM), vmem, vmem, vmem],
        out_specs=vmem,
        scratch_shapes=[
            halo,
            halo,
            pltpu.VMEM((n_tp, rows, window), jnp.float32),
            pltpu.VMEM((group * rows, window), jnp.float32),
            pltpu.VMEM((group * rows, LANES), jnp.float32),
            pltpu.VMEM((group * rows, window), jnp.bfloat16),
            pltpu.VMEM((kv_local, n_tp, rows, group * HEAD), jnp.bfloat16),
            dma((2, 2, kv_local, 3)),
            dma((2, 2, kv_local, 3)),
            dma((2, 2, kv_local, 6)),
            dma((kv_local, n_tp)),
            dma((kv_local, n_tp)),
        ],
        compiler_params=pltpu.CompilerParams(has_side_effects=True, collective_id=0, vmem_limit_bytes=60 * 1024 * 1024),
    )(doc_lengths, queries, keys, values)


def solution(mesh):
    in_specs = (P("cp", "tp"), P("cp", "tp"), P("cp", "tp"), P())
    return jax.shard_map(
        on_device, mesh=mesh, in_specs=in_specs, out_specs=P(("cp", "tp"), None), check_vma=False
    )
```

```python
import functools
import math

import jax
import jax.numpy as jnp
from jax import lax
from jax.experimental import pallas as pl
from jax.experimental.pallas import tpu as pltpu
from jax.sharding import PartitionSpec as P

HEAD = 128
BACK = 4
LANES = 128
negative = -1e30
MESH = pl.DeviceIdType.MESH


def kernel(
    n_cp, n_tp, group, kv_local,
    doc_ref, q_ref, k_ref, v_ref, out_ref,
    kbuf, vbuf, bias_ref, s_ref, mx_ref, p_ref, obuf,
    own_send, relay_send, kv_recv, o_send, o_recv,
):
    tok = q_ref.shape[0]
    half = tok // 2
    rows = tok // n_tp
    parts = half // rows
    window = bias_ref.shape[2]
    step = half * (BACK + 1) - window
    step = step // max(parts - 1, 1)
    cols = group * HEAD
    me = lax.axis_index("cp")
    tp = lax.axis_index("tp")
    core = me % 2
    chip = me // 2
    chips = n_cp // 2
    partner = me + 1 - 2 * core
    bufs = (kbuf, vbuf)
    srcs = (k_ref, v_ref)
    idx = (core, 1 - core)

    def part(kv, h, g, slot):
        return bufs[kv][g].at[h, pl.ds(pl.multiple_of(slot * half, half), half)]

    def src(kv, h, g):
        return srcs[kv].at[pl.ds(h * half, half), pl.ds(g * HEAD, HEAD)]

    def send(source, kv, h, g, slot, ssem, dev):
        return pltpu.make_async_remote_copy(
            src_ref=source,
            dst_ref=part(kv, h, g, slot),
            send_sem=ssem,
            recv_sem=kv_recv.at[kv, h, g, slot],
            device_id={"cp": dev},
            device_id_type=MESH,
        )

    routes = []
    for o in (2, 1):
        base = (2 - o) * 2
        routes.append((0, o, chip + o <= chips - 1, chip + o, 0, base + idx[0]))
        if o == 2:
            routes.append((0, o, chip == chips - 1, chips - 2, 1, base + idx[0]))
        routes.append((1, o, chip >= o, chip - o, 1, base + idx[1]))

    def own_copies(g, fn):
        for kv in range(2):
            for h, o, when, tchip, thalf, slot in routes:
                @pl.when(when)
                def _(kv=kv, h=h, o=o, tchip=tchip, thalf=thalf, slot=slot):
                    fn(send(src(kv, h, g), kv, thalf, g, slot, own_send.at[kv, h, g, o], 2 * tchip + core))
            for h in range(2):
                fn(send(src(kv, h, g), kv, h, g, 4 + idx[h], own_send.at[kv, h, g, 0], partner))

    arrivals = []
    for o in (2, 1):
        arrivals.append((0, o, chip >= o, core))
        arrivals.append((1, o, chip < chips - o, 1 - core))
        if o == 2:
            arrivals.append((1, o, chip == chips - 2, core))

    def relays(g, fn):
        for h, o, when, r in arrivals:
            @pl.when(when)
            def _(h=h, o=o, r=r):
                for kv in range(2):
                    slot = (2 - o) * 2 + r
                    fn(send(part(kv, h, g, slot), kv, h, g, slot, relay_send.at[kv, h, g, o], partner))

    def take(copy):
        copy.wait_recv()
        copy.start()

    def relay_arrivals(g):
        for h, o, when, r in arrivals:
            @pl.when(when)
            def _(h=h, o=o, r=r):
                for kv in range(2):
                    slot = (2 - o) * 2 + 1 - r
                    send(part(kv, h, g, slot), kv, h, g, slot, relay_send.at[kv, h, g, o], partner).wait_recv()
        for h in range(2):
            for kv in range(2):
                slot = 4 + 1 - idx[h]
                send(part(kv, h, g, slot), kv, h, g, slot, own_send.at[kv, h, g, 0], partner).wait_recv()

        @pl.when(chip == chips - 1)
        def _():
            for buf in bufs:
                buf[g][1, 0:4 * half] = buf[g][0, 2 * half:6 * half]

    barrier = pltpu.get_barrier_semaphore()
    greeted = n_tp
    pl.semaphore_signal(barrier, inc=1, device_id={"cp": partner}, device_id_type=MESH)
    for other in range(1, n_tp):
        pl.semaphore_signal(barrier, inc=1, device_id={"tp": (tp + other) % n_tp}, device_id_type=MESH)
    for away in (-2, -1, 1, 2):
        there = chip + away
        inside = (there >= 0) & (there < chips)
        greeted = greeted + inside.astype(jnp.int32)

        @pl.when(inside)
        def _(there=there):
            pl.semaphore_signal(barrier, inc=1, device_id={"cp": 2 * there + core}, device_id_type=MESH)
    pl.semaphore_wait(barrier, greeted)

    own_copies(0, lambda copy: copy.start())

    for g in range(kv_local):
        for h in range(2):
            for kv in range(2):
                part(kv, h, g, 4 + idx[h])[...] = srcs[kv][h * half:(h + 1) * half, g * HEAD:(g + 1) * HEAD]
        for lowest in range(2):
            @pl.when(chip <= lowest)
            def _(g=g, lowest=lowest):
                first = 2 if lowest == 0 else 0
                for buf in bufs:
                    buf[g][0, first * half:(first + 2) * half] = jnp.zeros((2 * half, HEAD), jnp.bfloat16)

    def place(u):
        h = u // parts
        i = u % parts
        pair = chip + h * (2 * chips - 1 - 2 * chip)
        index = core + h * (1 - 2 * core)
        return h, i, pair, index

    def make_bias(u, _):
        h, i, pair, index = place(u)
        block = 2 * pair + index
        q_pos = block * half + i * rows + lax.broadcasted_iota(jnp.int32, (rows, LANES), 0)

        def doc_step(j, carry):
            end, low = carry
            end = end + doc_ref[j]
            return end, jnp.where(end <= q_pos, end, low)

        _, low = lax.fori_loop(0, doc_ref.shape[0], doc_step, (jnp.int32(0), jnp.zeros((rows, LANES), jnp.int32)))
        first = (block - BACK) * half + i * step
        for tile in range(window // LANES):
            k_pos = first + tile * LANES + lax.broadcasted_iota(jnp.int32, (rows, LANES), 1)
            ok = (k_pos >= low) & (k_pos <= q_pos)
            bias_ref[u, :, tile * LANES:(tile + 1) * LANES] = jnp.where(ok, 0.0, negative)
        return 0

    lax.fori_loop(0, n_tp, make_bias, 0)

    chunk = 2 * LANES
    factor = float(HEAD) ** -0.5 * math.log2(math.e)

    def out_copy(g, u):
        return pltpu.make_async_remote_copy(
            src_ref=obuf.at[g, u],
            dst_ref=out_ref.at[:, pl.ds(pl.multiple_of(tp * (kv_local * cols) + g * cols, LANES), cols)],
            send_sem=o_send.at[g, u],
            recv_sem=o_recv.at[g, tp],
            device_id={"tp": u},
            device_id_type=MESH,
        )

    def out_arrival(g, source):
        return pltpu.make_async_remote_copy(
            src_ref=obuf.at[g, source],
            dst_ref=out_ref.at[:, pl.ds(pl.multiple_of(source * (kv_local * cols) + g * cols, LANES), cols)],
            send_sem=o_send.at[g, source],
            recv_sem=o_recv.at[g, source],
            device_id={"tp": source},
            device_id_type=MESH,
        )

    def attend(g, u):
        h, i, pair, index = place(u)
        row0 = pl.multiple_of(u * rows, 16)
        q = jnp.concatenate(
            [q_ref[pl.ds(row0, rows), (g * group + j) * HEAD:(g * group + j + 1) * HEAD] for j in range(group)], axis=0
        )
        start = index * half + i * step
        mx_ref[...] = jnp.full(mx_ref.shape, negative, jnp.float32)

        def score_chunk(kc, _):
            k = kbuf[g][h, pl.ds(pl.multiple_of(start + kc * chunk, LANES), chunk), :]
            s = lax.dot_general(q, k, (((1,), (1,)), ((), ())), preferred_element_type=jnp.float32)
            at = pl.ds(pl.multiple_of(kc * chunk, chunk), chunk)
            bias = bias_ref[u, :, at]
            for j in range(group):
                here = slice(j * rows, (j + 1) * rows)
                sj = s[here] + bias
                s_ref[here, at] = sj
                mx_ref[here] = jnp.maximum(mx_ref[here], jnp.maximum(sj[:, :LANES], sj[:, LANES:]))
            return 0

        lax.fori_loop(0, window // chunk, score_chunk, 0)
        tall = 64

        def weigh(rc, _):
            at = pl.ds(pl.multiple_of(rc * tall, tall), tall)
            top = jnp.max(mx_ref[at, :], axis=1, keepdims=True)
            p_ref[at, :] = jnp.exp2((s_ref[at, :] - top) * factor).astype(jnp.bfloat16)
            return 0

        lax.fori_loop(0, group * rows // tall, weigh, 0)
        v = vbuf[g][h, pl.ds(pl.multiple_of(start, LANES), window), :]
        wide = jnp.concatenate([v, jnp.ones_like(v)], axis=1)
        acc = jnp.dot(p_ref[...], wide, preferred_element_type=jnp.float32)
        done = (acc[:, :HEAD] / acc[:, HEAD:]).astype(jnp.bfloat16)
        for j in range(group):
            obuf[g, u, :, j * HEAD:(j + 1) * HEAD] = done[j * rows:(j + 1) * rows]

    def order(k):
        if n_tp != 4:
            return (tp + 1 + k) % n_tp
        far = (tp // 2 + 1 - k // 2) % 2
        return 2 * far + (tp % 2 + k + k // 2) % 2

    relays(0, take)
    for g in range(1, kv_local):
        own_copies(g, lambda copy: copy.start())
    relay_arrivals(0)
    for g in range(kv_local):
        def one(k, _, g=g):
            u = order(k)
            if g + 1 < kv_local:
                @pl.when(k == n_tp - 1)
                def _():
                    relays(g + 1, take)
            attend(g, u)

            @pl.when(k < n_tp - 1)
            def _():
                out_copy(g, u).start()
            return 0

        lax.fori_loop(0, n_tp, one, 0)
        out_ref[:, pl.ds(pl.multiple_of(tp * (kv_local * cols) + g * cols, LANES), cols)] = obuf[g, tp]
        if g + 1 < kv_local:
            relay_arrivals(g + 1)

    for g in range(kv_local):
        own_copies(g, lambda copy: copy.wait_send())
        relays(g, lambda copy: copy.wait_send())

        def finish(k, _, g=g):
            u = (tp + 1 + k) % n_tp
            out_copy(g, u).wait_send()
            out_arrival(g, u).wait_recv()
            return 0

        lax.fori_loop(0, n_tp - 1, finish, 0)


def on_device(queries, keys, values, doc_lengths):
    tok, q_cols = queries.shape
    kv_local = keys.shape[1] // HEAD
    group = q_cols // keys.shape[1]
    n_cp = lax.axis_size("cp")
    n_tp = lax.axis_size("tp")
    half = tok // 2
    rows = tok // n_tp
    window = -(-(BACK * half + rows) // (2 * LANES)) * 2 * LANES
    vmem = pl.BlockSpec(memory_space=pltpu.VMEM)
    dma = pltpu.SemaphoreType.DMA
    halo = (pltpu.VMEM((2, 6 * half, HEAD), jnp.bfloat16),) * kv_local
    return pl.pallas_call(
        functools.partial(kernel, n_cp, n_tp, group, kv_local),
        out_shape=jax.ShapeDtypeStruct((rows, q_cols * n_tp), jnp.bfloat16),
        in_specs=[pl.BlockSpec(memory_space=pltpu.SMEM), vmem, vmem, vmem],
        out_specs=vmem,
        scratch_shapes=[
            halo,
            halo,
            pltpu.VMEM((n_tp, rows, window), jnp.float32),
            pltpu.VMEM((group * rows, window), jnp.float32),
            pltpu.VMEM((group * rows, LANES), jnp.float32),
            pltpu.VMEM((group * rows, window), jnp.bfloat16),
            pltpu.VMEM((kv_local, n_tp, rows, group * HEAD), jnp.bfloat16),
            dma((2, 2, kv_local, 3)),
            dma((2, 2, kv_local, 3)),
            dma((2, 2, kv_local, 6)),
            dma((kv_local, n_tp)),
            dma((kv_local, n_tp)),
        ],
        compiler_params=pltpu.CompilerParams(has_side_effects=True, collective_id=0, vmem_limit_bytes=44 * 1024 * 1024),
    )(doc_lengths, queries, keys, values)


def solution(mesh):
    in_specs = (P("cp", "tp"), P("cp", "tp"), P("cp", "tp"), P())
    return jax.shard_map(
        on_device, mesh=mesh, in_specs=in_specs, out_specs=P(("cp", "tp"), None), check_vma=False
    )
```
